16 devices in a mesh: rep: 1, dp: 16 (over x, y, z, core).
Axes of the slice: x: 2, y: 2, z: 2, core: 2. Of those that a mesh axis runs over, the one named last changes fastest.
Arguments:
- a: bfloat16 [16, 4, 4096, 1024], P(('rep', 'dp'))
- g: bfloat16 [16, 4, 4096, 4096], P(('rep', 'dp'))
Outputs:
- output: bfloat16 [4, 1024, 4096], P('rep')
All inputs are finite; a program needn't handle non-finite values.
Results may differ from the reference program's by a relative error of at most 0.012.
Values are sent between devices in bfloat16 or wider.
A program may use at most 2 GiB of HBM per device.

```python
import jax
import jax.numpy as jnp
from jax import lax

DEVICES = 16
MATRICES = 4
TOKENS = 4096
D = 1024
FF = 4096


def setup_inputs(seed: int = 0, part: int = 0) -> dict:
    ka, kg, ks = (jax.random.fold_in(k, part) for k in jax.random.split(jax.random.key(seed), 3))
    size = 2.0 ** jax.random.uniform(ks, (DEVICES, MATRICES, 1, 1), jnp.float32, -1.0, 1.0)
    a = jax.random.normal(ka, (DEVICES, MATRICES, TOKENS, D), jnp.float32)
    g = size * jax.random.normal(kg, (DEVICES, MATRICES, TOKENS, FF), jnp.float32) * (DEVICES * TOKENS) ** -0.5
    return {"a": a.astype(jnp.bfloat16), "g": g.astype(jnp.bfloat16)}


def reference(a, g):
    def take(so_far, one):
        return so_far + jnp.einsum("ntd,ntf->ndf", *one, preferred_element_type=jnp.float32), None

    return lax.scan(take, jnp.zeros((MATRICES, D, FF), jnp.float32), (a, g))[0].astype(jnp.bfloat16)
```

```python
import functools

import jax
import jax.numpy as jnp
from jax import lax
from jax.experimental import pallas as pl
from jax.experimental.pallas import tpu as pltpu
from jax.sharding import PartitionSpec as P

MESH = pl.DeviceIdType.MESH
BF16, F32 = jnp.bfloat16, jnp.float32

MATS, TOKENS, D, F = 4, 4096, 1024, 4096
FB = 512
NJ = F // FB
NCH = MATS * NJ
VLIM = 26 * 2**20
NB = 256
HALF = D // 2
SR = 6
SS = 3
R, ROT = 2, 1
LAG = 3
NUM, DEN, T0 = 3, 3, 3 * R + 1


def kernel(a_hbm, g_hbm, out0, out1, abuf, gbuf, acc, sbuf, rbuf, k1, k2, k3, s1, s2, s3, r1, r2, r3,
           asem, gsem, dsend, drecv, rsend, rrecv, gsend, grecv):
    me = lax.axis_index("dp")
    core = me % 2
    bits = [(me // 8) % 2, (me // 4) % 2, (me // 2) % 2]
    mates = [me + (1 - 2 * b) * w for b, w in zip(bits, (8, 4, 2))]
    twin = me + 1 - 2 * core
    own = core * HALF

    def pick(which, values):
        return jnp.where(which == 0, values[0], jnp.where(which == 1, values[1], values[2]))

    def order(c, step):
        axis = (ROT * c + core + step) % 3
        return pick(axis, bits), pick(axis, mates)

    def remote(src, dst, send, recv, to):
        return pltpu.make_async_remote_copy(
            src_ref=src, dst_ref=dst, send_sem=send, recv_sem=recv, device_id={"dp": to}, device_id_type=MESH
        )

    def place(c):
        return c // NJ, pl.multiple_of((c % NJ) * FB, FB)

    def load_a(n, half):
        col = pl.multiple_of(jnp.where(half == 0, HALF - own, own), HALF)
        return pltpu.make_async_copy(a_hbm.at[n, :, pl.ds(col, HALF)], abuf.at[half], asem.at[half])

    def load_g(c):
        n, col = place(c)
        return pltpu.make_async_copy(g_hbm.at[n, :, pl.ds(col, FB)], gbuf.at[c % 2], gsem.at[c % 2])

    def twin_copy(c):
        return remote(sbuf.at[c % 2], rbuf.at[c % 2], dsend.at[c % 2], drecv.at[c % 2], twin)

    def scatter_copy(c, step):
        _, to = order(c, step)
        src, dst = ((s1, r1), (s2, r2), (s3, r3))[step]
        return remote(src.at[c % SS], dst.at[c % SR], rsend.at[step, c % SS], rrecv.at[step, c % SR], to)

    def piece(c):
        b1, b2, b3 = (order(c, s)[0] for s in range(3))
        return b1, b2, b3

    def rows_of(c, step):
        b1, b2, b3 = piece(c)
        if step == 0:
            return pl.ds(pl.multiple_of(own + b1 * 256 + b2 * 128 + b3 * 64, 64), 64)
        if step == 1:
            return pl.ds(pl.multiple_of(own + b1 * 256 + b2 * 128, 128), 128)
        if step == 2:
            return pl.ds(pl.multiple_of(own + b1 * 256, 256), 256)
        return pl.ds(pl.multiple_of(own, HALF), HALF)

    def gather_copy(c, step, out=out0, m=0):
        _, col = place(c)
        to = twin if step == 3 else order(c, 2 - step)[1]
        where = out.at[m, rows_of(c, step), pl.ds(col, FB)]
        return remote(where, where, gsend.at[step, c], grecv.at[step, c], to)

    def on_out(c, do):
        @pl.when(c < NJ)
        def _():
            do(out0, 0)

        @pl.when(c >= NJ)
        def _():
            do(out1, c // NJ - 1)

    def dots(c, half, store):
        for j in range(FB // NB):
            cols = slice(j * NB, (j + 1) * NB)
            store(cols, lax.dot_general(
                abuf[half], gbuf[c % 2, :, cols], (((0,), (0,)), ((), ())), preferred_element_type=F32))

    def store_send(c):
        def store(cols, x):
            sbuf[c % 2, :, cols] = x.astype(BF16)
        return store

    def store_own(cols, x):
        acc[:, cols] = x

    def halves(c, step, size):
        b, _ = order(c, step)
        return (pl.ds(pl.multiple_of((1 - b) * size, size), size), pl.ds(pl.multiple_of(b * size, size), size))

    def split(c, step, mine, theirs, send, keep, size):
        away, stay = halves(c, step, size)
        @pl.when(c >= SS)
        def _():
            scatter_copy(c - SS, step).wait_send()
        send[c % SS] = (mine[away] + theirs[away].astype(F32)).astype(BF16)
        scatter_copy(c, step).start()
        keep[c % R] = mine[stay] + theirs[stay].astype(F32)

    def reduce_round(t):
        c = t - 3 * R
        @pl.when((c >= 0) & (c < NCH))
        def _():
            scatter_copy(c, 2).wait_recv()
            _, col = place(c)
            total = (k3[c % R] + r3[c % SR].astype(F32)).astype(BF16)
            def put(out, m):
                out[m, rows_of(c, 0), pl.ds(col, FB)] = total
            on_out(c, put)
        for step, c, mine, recv, send, keep, size in (
            (2, t - 2 * R, k2, r2, s3, k3, 64),
            (1, t - R, k1, r1, s2, k2, 128),
        ):
            @pl.when((c >= 0) & (c < NCH))
            def _():
                scatter_copy(c, step - 1).wait_recv()
                split(c, step, mine.at[c % R], recv.at[c % SR], send, keep, size)
        @pl.when(t < NCH)
        def _():
            twin_copy(t).wait_recv()
            split(t, 0, acc, rbuf.at[t % 2], s1, k1, 256)

    def gather_round(u):
        for step in (3, 2, 1, 0):
            c = u - LAG * step
            @pl.when((c >= 0) & (c < NCH))
            def _():
                if step:
                    gather_copy(c, step - 1).wait_recv()
                on_out(c, lambda out, m: gather_copy(c, step, out, m).start())

    def rounds_before(t):
        return jnp.maximum(t - T0, 0) * NUM // DEN

    for half in range(2):
        load_a(0, half).start()
    load_g(0).start()

    barrier = pltpu.get_barrier_semaphore()
    for to in (*mates, twin):
        pl.semaphore_signal(barrier, inc=1, device_id={"dp": to}, device_id_type=MESH)
    pl.semaphore_wait(barrier, 4)

    @pl.loop(0, NCH)
    def _(t):
        n, j = t // NJ, t % NJ
        load_g(t).wait()
        @pl.when(t + 1 < NCH)
        def _():
            load_g(t + 1).start()
        for half in range(2):
            @pl.when(j == 0)
            def _():
                load_a(n, half).wait()
            if half == 0:
                @pl.when(t >= 2)
                def _():
                    twin_copy(t - 2).wait_send()
                dots(t, 0, store_send(t))
                twin_copy(t).start()
            else:
                dots(t, 1, store_own)
            @pl.when((j == NJ - 1) & (n < MATS - 1))
            def _():
                load_a(n + 1, half).start()
        reduce_round(t)
        u = rounds_before(t)
        @pl.when(rounds_before(t + 1) > u)
        def _():
            gather_round(u)

    first = max(NCH - T0, 0) * NUM // DEN

    @pl.loop(first, NCH + 3 * LAG)
    def _(u):
        t = u - first + NCH
        @pl.when(t < NCH + 3 * R)
        def _():
            reduce_round(t)
        gather_round(u)

    for c in range(NCH - 2, NCH):
        twin_copy(c).wait_send()
    for step in range(3):
        for c in range(NCH - SS, NCH):
            scatter_copy(c, step).wait_send()

    @pl.loop(0, NCH)
    def _(c):
        for step in range(4):
            gather_copy(c, step).wait_send()
        gather_copy(c, 3).wait_recv()


def gather_up(out0, out1, out, sem):
    copies = [
        pltpu.make_async_copy(src, out.at[n], sem.at[n])
        for n, src in enumerate((out0.at[0], out1.at[0], out1.at[1], out1.at[2]))
    ]
    for copy in copies:
        copy.start()
    for copy in copies:
        copy.wait()


def solution(mesh):
    def body(a, g):
        vmem = pltpu.VMEM
        dma = pltpu.SemaphoreType.DMA
        hbm, near = pl.BlockSpec(memory_space=pl.ANY), pl.BlockSpec(memory_space=vmem)
        parts = pl.pallas_call(
            kernel,
            name="sums",
            out_shape=[vmem((1, D, F), BF16), vmem((MATS - 1, D, F), BF16)],
            in_specs=[hbm] * 2,
            out_specs=[near] * 2,
            scratch_shapes=[
                vmem((2, TOKENS, HALF), BF16),
                vmem((2, TOKENS, FB), BF16),
                vmem((HALF, FB), F32),
                vmem((2, HALF, FB), BF16),
                vmem((2, HALF, FB), BF16),
                vmem((R, 256, FB), F32),
                vmem((R, 128, FB), F32),
                vmem((R, 64, FB), F32),
                vmem((SS, 256, FB), BF16),
                vmem((SS, 128, FB), BF16),
                vmem((SS, 64, FB), BF16),
                vmem((SR, 256, FB), BF16),
                vmem((SR, 128, FB), BF16),
                vmem((SR, 64, FB), BF16),
                dma((2,)), dma((2,)), dma((2,)), dma((2,)),
                dma((3, SS)), dma((3, SR)),
                dma((4, NCH)), dma((4, NCH)),
            ],
            compiler_params=pltpu.CompilerParams(
                collective_id=0, has_side_effects=True, vmem_limit_bytes=VLIM
            ),
        )(a[0], g[0])
        return pl.pallas_call(
            gather_up,
            name="gather_up",
            out_shape=jax.ShapeDtypeStruct((MATS, D, F), BF16),
            in_specs=[near] * 2,
            out_specs=hbm,
            scratch_shapes=[dma((4,))],
            compiler_params=pltpu.CompilerParams(vmem_limit_bytes=2**20),
        )(*parts)

    return jax.shard_map(
        body, mesh=mesh, in_specs=P(("rep", "dp")), out_specs=P("rep"), check_vma=False
    )
```

```python
import functools

import jax
import jax.numpy as jnp
from jax import lax
from jax.experimental import pallas as pl
from jax.experimental.pallas import tpu as pltpu
from jax.sharding import PartitionSpec as P

MESH = pl.DeviceIdType.MESH
BF16, F32 = jnp.bfloat16, jnp.float32

MATS, TOKENS, D, F = 4, 4096, 1024, 4096
FB = 512
RB = 256
NJ, NH = F // FB, D // 2 // RB
NM = NJ * NH
NCH = MATS * NM
VLIM = 26 * 2**20
NB = 512
HALF = D // 2
SR = 6
SS = 3
R, ROT = 2, 1
LAG = 3
T0 = 3 * R


class At:
    def __init__(self, value, rest):
        self.value, self.rest = value, rest % 6

    def __sub__(self, k):
        return At(self.value - k, self.rest - k)

    def __mod__(self, k):
        assert 6 % k == 0
        return self.rest % k


def kernel(a_hbm, g_hbm, out0, out1, abuf, gbuf, acc, sbuf, rbuf, k1, k2, k3, s1, s2, s3, r1, r2, r3,
           asem, gsem, dsend, drecv, rsend, rrecv, gsend, grecv):
    me = lax.axis_index("dp")
    core = me % 2
    bits = [(me // 8) % 2, (me // 4) % 2, (me // 2) % 2]
    mates = [me + (1 - 2 * b) * w for b, w in zip(bits, (8, 4, 2))]
    twin = me + 1 - 2 * core
    own = core * HALF

    def pick(which, values):
        return jnp.where(which == 0, values[0], jnp.where(which == 1, values[1], values[2]))

    ways = [(pick((k + core) % 3, bits), pick((k + core) % 3, mates)) for k in range(3)]

    def order(c, step):
        return ways[(ROT * c.rest + step) % 3]

    def remote(src, dst, send, recv, to):
        return pltpu.make_async_remote_copy(
            src_ref=src, dst_ref=dst, send_sem=send, recv_sem=recv, device_id={"dp": to}, device_id_type=MESH
        )

    def place(c):
        c = c.value
        return c // NM, pl.multiple_of((c % NM) // NH * FB, FB), pl.multiple_of(own + c % NH * RB, RB)

    def load_a(n, half):
        col = pl.multiple_of(jnp.where(half == 0, HALF - own, own), HALF)
        return pltpu.make_async_copy(a_hbm.at[n, :, pl.ds(col, HALF)], abuf.at[half], asem.at[half])

    def load_g(c):
        n, col, _ = place(c)
        slot = c.value // NH % 2
        return pltpu.make_async_copy(g_hbm.at[n, :, pl.ds(col, FB)], gbuf.at[slot], gsem.at[slot])

    def twin_copy(c):
        return remote(sbuf.at[c % 2], rbuf.at[c % 2], dsend.at[c % 2], drecv.at[c % 2], twin)

    def scatter_copy(c, step):
        _, to = order(c, step)
        src, dst = ((s1, r1), (s2, r2), (s3, r3))[step]
        return remote(src.at[c % SS], dst.at[c % SR], rsend.at[step, c % SS], rrecv.at[step, c % SR], to)

    def piece(c):
        b1, b2, b3 = (order(c, s)[0] for s in range(3))
        return b1, b2, b3

    def rows_of(c, step):
        b1, b2, b3 = piece(c)
        base = place(c)[2]
        if step == 0:
            return pl.ds(pl.multiple_of(base + b1 * (RB // 2) + b2 * (RB // 4) + b3 * (RB // 8), RB // 8), RB // 8)
        if step == 1:
            return pl.ds(pl.multiple_of(base + b1 * (RB // 2) + b2 * (RB // 4), RB // 4), RB // 4)
        if step == 2:
            return pl.ds(pl.multiple_of(base + b1 * (RB // 2), RB // 2), RB // 2)
        return pl.ds(base, RB)

    def gather_copy(c, step, out=out0, m=0):
        _, col, _ = place(c)
        to = twin if step == 3 else order(c, 2 - step)[1]
        where = out.at[m, rows_of(c, step), pl.ds(col, FB)]
        return remote(where, where, gsend.at[step, c.value], grecv.at[step, c.value], to)

    def on_out(c, do):
        @pl.when(c.value < NM)
        def _():
            do(out0, 0)

        @pl.when(c.value >= NM)
        def _():
            do(out1, c.value // NM - 1)

    def dots(c, half, store):
        for j in range(FB // NB):
            cols = slice(j * NB, (j + 1) * NB)
            store(cols, lax.dot_general(
                abuf[half, :, pl.ds(c % NH * RB, RB)], gbuf[c.value // NH % 2, :, cols], (((0,), (0,)), ((), ())), preferred_element_type=F32))

    def store_send(c):
        def store(cols, x):
            sbuf[c % 2, :, cols] = x.astype(BF16)
        return store

    def store_own(cols, x):
        acc[:, cols] = x

    def halves(c, step, size):
        b, _ = order(c, step)
        return (pl.ds(pl.multiple_of((1 - b) * size, size), size), pl.ds(pl.multiple_of(b * size, size), size))

    def split(c, step, mine, theirs, send, keep, size):
        away, stay = halves(c, step, size)
        @pl.when(c.value >= SS)
        def _():
            scatter_copy(c - SS, step).wait_send()
        send[c % SS] = (mine[away] + theirs[away].astype(F32)).astype(BF16)
        scatter_copy(c, step).start()
        keep[c % R] = mine[stay] + theirs[stay].astype(F32)

    def reduce_round(t):
        c = t - 3 * R
        @pl.when((c.value >= 0) & (c.value < NCH))
        def _():
            scatter_copy(c, 2).wait_recv()
            _, col, _ = place(c)
            total = (k3[c % R] + r3[c % SR].astype(F32)).astype(BF16)
            def put(out, m):
                out[m, rows_of(c, 0), pl.ds(col, FB)] = total
            on_out(c, put)
        for step, c, mine, recv, send, keep, size in (
            (2, t - 2 * R, k2, r2, s3, k3, RB // 8),
            (1, t - R, k1, r1, s2, k2, RB // 4),
        ):
            @pl.when((c.value >= 0) & (c.value < NCH))
            def _():
                scatter_copy(c, step - 1).wait_recv()
                split(c, step, mine.at[c % R], recv.at[c % SR], send, keep, size)
        @pl.when(t.value < NCH)
        def _():
            twin_copy(t).wait_recv()
            split(t, 0, acc, rbuf.at[t % 2], s1, k1, RB // 2)

    def gather_round(u):
        for step in (3, 2, 1, 0):
            c = u - LAG * step
            @pl.when((c.value >= 0) & (c.value < NCH))
            def _():
                if step:
                    gather_copy(c, step - 1).wait_recv()
                on_out(c, lambda out, m: gather_copy(c, step, out, m).start())

    for half in range(2):
        load_a(0, half).start()
    load_g(At(0, 0)).start()

    barrier = pltpu.get_barrier_semaphore()
    for to in (*mates, twin):
        pl.semaphore_signal(barrier, inc=1, device_id={"dp": to}, device_id_type=MESH)
    pl.semaphore_wait(barrier, 4)

    def multiply(t):
        n, j = t.value // NM, t.value % NM

        if t % NH == 0:
            load_g(t).wait()

            @pl.when(t.value + NH < NCH)
            def _():
                load_g(t - -NH).start()

        for half in range(2):
            @pl.when(j == 0)
            def _():
                load_a(n, half).wait()
            if half == 0:
                @pl.when(t.value >= 2)
                def _():
                    twin_copy(t - 2).wait_send()
                dots(t, 0, store_send(t))
                twin_copy(t).start()
            else:
                dots(t, 1, store_own)
            @pl.when((j == NM - 1) & (n < MATS - 1))
            def _():
                load_a(n + 1, half).start()

    @pl.loop(0, pl.cdiv(max(NCH + 3 * R, NCH + T0 + 3 * LAG), 6))
    def _(q):
        for r in range(6):
            t = At(6 * q + r, r)

            @pl.when(t.value < NCH)
            def _():
                multiply(t)
            reduce_round(t)
            gather_round(t - T0)

    for c in range(NCH - 2, NCH):
        twin_copy(At(c, c)).wait_send()
    for step in range(3):
        for c in range(NCH - SS, NCH):
            scatter_copy(At(c, c), step).wait_send()

    @pl.loop(0, NCH)
    def _(c):
        for step in range(4):
            gather_copy(At(c, 0), step).wait_send()
        gather_copy(At(c, 0), 3).wait_recv()


def gather_up(out0, out1, out, sem):
    copies = [
        pltpu.make_async_copy(src, out.at[n], sem.at[n])
        for n, src in enumerate((out0.at[0], out1.at[0], out1.at[1], out1.at[2]))
    ]
    for copy in copies:
        copy.start()
    for copy in copies:
        copy.wait()


def solution(mesh):
    def body(a, g):
        vmem = pltpu.VMEM
        dma = pltpu.SemaphoreType.DMA
        hbm, near = pl.BlockSpec(memory_space=pl.ANY), pl.BlockSpec(memory_space=vmem)
        parts = pl.pallas_call(
            kernel,
            name="sums",
            out_shape=[vmem((1, D, F), BF16), vmem((MATS - 1, D, F), BF16)],
            in_specs=[hbm] * 2,
            out_specs=[near] * 2,
            scratch_shapes=[
                vmem((2, TOKENS, HALF), BF16),
                vmem((2, TOKENS, FB), BF16),
                vmem((RB, FB), F32),
                vmem((2, RB, FB), BF16),
                vmem((2, RB, FB), BF16),
                vmem((R, RB // 2, FB), F32),
                vmem((R, RB // 4, FB), F32),
                vmem((R, RB // 8, FB), F32),
                vmem((SS, RB // 2, FB), BF16),
                vmem((SS, RB // 4, FB), BF16),
                vmem((SS, RB // 8, FB), BF16),
                vmem((SR, RB // 2, FB), BF16),
                vmem((SR, RB // 4, FB), BF16),
                vmem((SR, RB // 8, FB), BF16),
                dma((2,)), dma((2,)), dma((2,)), dma((2,)),
                dma((3, SS)), dma((3, SR)),
                dma((4, NCH)), dma((4, NCH)),
            ],
            compiler_params=pltpu.CompilerParams(
                collective_id=0, has_side_effects=True, vmem_limit_bytes=VLIM
            ),
        )(a[0], g[0])
        return pl.pallas_call(
            gather_up,
            name="gather_up",
            out_shape=jax.ShapeDtypeStruct((MATS, D, F), BF16),
            in_specs=[near] * 2,
            out_specs=hbm,
            scratch_shapes=[dma((4,))],
            compiler_params=pltpu.CompilerParams(vmem_limit_bytes=2**20),
        )(*parts)

    return jax.shard_map(
        body, mesh=mesh, in_specs=P(("rep", "dp")), out_specs=P("rep"), check_vma=False
    )
```
